256 devices in a mesh: row: 16 (over z, core), col: 16 (over x, y).
Axes of the slice: x: 4, y: 4, z: 8, core: 2. Of those that a mesh axis runs over, the one named last changes fastest.
Arguments:
- features: bfloat16 [16, 16, 1024, 602], P('row', 'col'), may hold values from -6 to 6
- local_mask: int32 [16, 16, 1024, 1024], P('row', 'col'), may hold values 0 or 1
- halo_mask: int32 [16, 16, 1024, 512], P('row', 'col'), may hold values 0 or 1
- boundary_index: int32 [16, 16, 512], P('row', 'col'), may hold values from 0 to 1023
- labels: int32 [16, 16, 1024], P('row', 'col'), may hold values from 0 to 40
- halo_first: bfloat16 [16, 16, 512, 602], P('row', 'col'), may hold values from -6 to 6
- halo_second: bfloat16 [16, 16, 512, 256], P('row', 'col'), may hold values from -4 to 4
- halo_third: bfloat16 [16, 16, 512, 256], P('row', 'col'), may hold values from -4 to 4
- return_second: bfloat16 [16, 16, 512, 256], P('row', 'col'), may hold values from -0.0059814453 to 0.0059814453
- return_third: bfloat16 [16, 16, 512, 256], P('row', 'col'), may hold values from -0.0059814453 to 0.0059814453
- weight_first: bfloat16 [602, 256], replicated, may hold values from -1 to 1
- weight_second: bfloat16 [256, 256], replicated, may hold values from -1.5 to 1.5
- weight_third: bfloat16 [256, 41], replicated, may hold values from -1.5 to 1.5
Outputs:
- grad_first: float32 [602, 256], replicated
- grad_second: float32 [256, 256], replicated
- grad_third: float32 [256, 41], replicated
- next_second: bfloat16 [16, 16, 512, 256], P('row', 'col')
- next_third: bfloat16 [16, 16, 512, 256], P('row', 'col')
- back_second: bfloat16 [16, 16, 512, 256], P('row', 'col')
- back_third: bfloat16 [16, 16, 512, 256], P('row', 'col')
The draws below stay inside these ranges and needn't reach their ends.
All inputs are finite; a program needn't handle non-finite values. No bound on the sum of `local_mask` or of `halo_mask` on one device may be relied on, other than what follows from the above.
Results may differ from the reference program's by a relative error of at most 0.007.
Values may be sent and summed in bfloat16 or wider, within the bound.
No kernel may reach another device: no remote copies, remote signals or barrier semaphores. Data moves between devices by JAX's collectives and lax.ppermute only.
A program may use at most 64 MiB of HBM per device.

```python
import jax
import jax.numpy as jnp
from jax import lax

IN_DIM = 602
HIDDEN_SIZE = 256
CLASSES = 41
NODE_DEV = 1024
BOUND = 128
N_ROW = 16
N_COL = 16


def place_ends(drawn, key, smallest, top_value):
    index_at = [jax.random.randint(jax.random.fold_in(key, axis), (), 0, length) for axis, length in enumerate(drawn.shape)]
    widest = drawn.shape.index(max(drawn.shape))
    neighbour = index_at[:widest] + [(index_at[widest] + 1) % drawn.shape[widest]] + index_at[widest + 1:]
    return drawn.at[tuple(index_at)].set(smallest).at[tuple(neighbour)].set(top_value)


def level_of(rng, dims, cuts, smallest, top_value):
    def one(dim, blocks):
        steps = jax.random.uniform(jax.random.fold_in(jax.random.fold_in(rng, 6), dim), (blocks,), jnp.float32, smallest / len(cuts), top_value / len(cuts))
        return jnp.repeat(jnp.exp(steps), dims[dim] // blocks).reshape((-1,) + (1,) * (len(dims) - dim - 1))

    level = one(*cuts[0])
    for cut in cuts[1:]:
        level = level * one(*cut)
    return level


def bell_draw(rng, dims, scale, bound, cuts=(), held_as=jnp.bfloat16):
    entries = scale * jax.random.normal(rng, dims, jnp.float32)
    if cuts:
        entries = entries * level_of(rng, dims, cuts, -0.22, 0.18)
    return jnp.clip(entries, -bound, bound).astype(held_as)


def setup_inputs(seed: int = 0) -> dict:
    keys = jax.random.split(jax.random.key(seed), 14)
    return {
        "features": bell_draw(keys[0], (N_ROW, N_COL, NODE_DEV, IN_DIM), 1.0, 6.0, ((0, 16), (1, 16))),
        "local_mask": place_ends((jax.random.randint(keys[1], (N_ROW, N_COL, NODE_DEV, NODE_DEV), 0, NODE_DEV) < min(16, NODE_DEV // 4)).astype(jnp.int32), jax.random.fold_in(keys[1], 1), 0, 1),
        "halo_mask": place_ends((jax.random.randint(keys[2], (N_ROW, N_COL, NODE_DEV, 4 * BOUND), 0, BOUND) < min(2, BOUND // 4)).astype(jnp.int32), jax.random.fold_in(keys[2], 1), 0, 1),
        "boundary_index": place_ends(jax.random.randint(keys[3], (N_ROW, N_COL, 4 * BOUND), 0, NODE_DEV), jax.random.fold_in(keys[3], 1), 0, NODE_DEV - 1).astype(jnp.int32),
        "labels": place_ends(jax.random.randint(keys[4], (N_ROW, N_COL, NODE_DEV), 0, CLASSES), jax.random.fold_in(keys[4], 1), 0, CLASSES - 1).astype(jnp.int32),
        "halo_first": bell_draw(keys[5], (N_ROW, N_COL, 4 * BOUND, IN_DIM), 1.0, 6.0, ((0, 16), (1, 16))),
        "halo_second": bell_draw(keys[6], (N_ROW, N_COL, 4 * BOUND, HIDDEN_SIZE), 0.5, 4.0, ((0, 16), (1, 16))),
        "halo_third": bell_draw(keys[7], (N_ROW, N_COL, 4 * BOUND, HIDDEN_SIZE), 0.5, 4.0, ((0, 16), (1, 16))),
        "return_second": bell_draw(keys[8], (N_ROW, N_COL, 4 * BOUND, HIDDEN_SIZE), 0.001, 0.0059814453, ((0, 16), (1, 16))),
        "return_third": bell_draw(keys[9], (N_ROW, N_COL, 4 * BOUND, HIDDEN_SIZE), 0.001, 0.0059814453, ((0, 16), (1, 16))),
        "weight_first": bell_draw(keys[10], (IN_DIM, HIDDEN_SIZE), (IN_DIM // 16) ** -0.5, 1.0),
        "weight_second": bell_draw(keys[11], (HIDDEN_SIZE, HIDDEN_SIZE), (HIDDEN_SIZE // 16) ** -0.5, 1.5),
        "weight_third": bell_draw(keys[12], (HIDDEN_SIZE, CLASSES), (HIDDEN_SIZE // 16) ** -0.5, 1.5),
    }


def slope(pre):
    sigma = jax.nn.sigmoid(pre)
    return sigma * (1.0 + pre * (1.0 - sigma))


def spread(local_bf, halo_bf, inverse, values, remote):
    summed = jnp.dot(local_bf, values, preferred_element_type=jnp.float32)
    summed = summed + values.astype(jnp.float32)
    summed = summed + jnp.dot(halo_bf, remote, preferred_element_type=jnp.float32)
    return (summed * inverse).astype(jnp.bfloat16)


def retract(local_bf, halo_bf, inverse, upstream, weight, hits, returned):
    across = jnp.dot(upstream, weight.T, preferred_element_type=jnp.float32)
    scaled = (across * inverse).astype(jnp.bfloat16)
    carried = jnp.dot(local_bf.T, scaled, preferred_element_type=jnp.float32) + scaled.astype(jnp.float32)
    carried = carried + jnp.dot(hits, returned, preferred_element_type=jnp.float32)
    outgoing = jnp.dot(halo_bf.T, scaled, preferred_element_type=jnp.float32).astype(jnp.bfloat16)
    return carried, outgoing


def partition(features, local_mask, halo_mask, boundary_index, labels, halo_first, halo_second, halo_third,
              return_second, return_third, weight_first, weight_second, weight_third):
    local_bf = local_mask.astype(jnp.bfloat16)
    halo_bf = halo_mask.astype(jnp.bfloat16)
    degree = 1.0 + jnp.sum(local_mask, axis=1).astype(jnp.float32) + jnp.sum(halo_mask, axis=1).astype(jnp.float32)
    inverse = (1.0 / degree)[:, None]
    node_rows = features.shape[0]
    hits = (jnp.arange(node_rows, dtype=jnp.int32)[:, None] == boundary_index[None, :]).astype(jnp.bfloat16)
    mixed_one = spread(local_bf, halo_bf, inverse, features, halo_first)
    pre_one = jnp.dot(mixed_one, weight_first, preferred_element_type=jnp.float32)
    hidden_one = jax.nn.silu(pre_one).astype(jnp.bfloat16)
    mixed_two = spread(local_bf, halo_bf, inverse, hidden_one, halo_second)
    pre_two = jnp.dot(mixed_two, weight_second, preferred_element_type=jnp.float32)
    hidden_two = jax.nn.silu(pre_two).astype(jnp.bfloat16)
    mixed_three = spread(local_bf, halo_bf, inverse, hidden_two, halo_third)
    logits = jnp.dot(mixed_three, weight_third, preferred_element_type=jnp.float32)
    expo = jnp.exp(logits)
    probs = expo / jnp.sum(expo, axis=1, keepdims=True)
    target = (labels[:, None] == jnp.arange(logits.shape[1], dtype=jnp.int32)[None, :]).astype(jnp.float32)
    upstream_three = ((probs - target) / node_rows).astype(jnp.bfloat16)
    grad_three = jnp.dot(mixed_three.T, upstream_three, preferred_element_type=jnp.float32)
    carried_two, outgoing_three = retract(local_bf, halo_bf, inverse, upstream_three, weight_third, hits, return_third)
    upstream_two = (carried_two * slope(pre_two)).astype(jnp.bfloat16)
    grad_two = jnp.dot(mixed_two.T, upstream_two, preferred_element_type=jnp.float32)
    carried_one, outgoing_two = retract(local_bf, halo_bf, inverse, upstream_two, weight_second, hits, return_second)
    upstream_one = (carried_one * slope(pre_one)).astype(jnp.bfloat16)
    grad_one = jnp.dot(mixed_one.T, upstream_one, preferred_element_type=jnp.float32)
    sent_second = jnp.take(hidden_one, boundary_index, axis=0)
    sent_third = jnp.take(hidden_two, boundary_index, axis=0)
    return grad_one, grad_two, grad_three, sent_second, sent_third, outgoing_two, outgoing_three


def route(sent):
    parted = sent.reshape((N_ROW, N_COL, 4, BOUND, sent.shape[-1]))
    blank_row = jnp.zeros_like(parted[:1, :, 0])
    blank_col = jnp.zeros_like(parted[:, :1, 0])
    from_above = jnp.concatenate([blank_row, parted[:-1, :, 1]], axis=0)
    from_below = jnp.concatenate([parted[1:, :, 0], blank_row], axis=0)
    from_left = jnp.concatenate([blank_col, parted[:, :-1, 3]], axis=1)
    from_right = jnp.concatenate([parted[:, 1:, 2], blank_col], axis=1)
    return jnp.stack([from_above, from_below, from_left, from_right], axis=2).reshape(sent.shape)


def reference(features, local_mask, halo_mask, boundary_index, labels, halo_first, halo_second, halo_third,
              return_second, return_third, weight_first, weight_second, weight_third):
    partitions = N_ROW * N_COL

    def flatten(array):
        return array.reshape((partitions,) + array.shape[2:])

    def advance(totals, pieces):
        result = partition(*pieces, weight_first, weight_second, weight_third)
        return (totals[0] + result[0], totals[1] + result[1], totals[2] + result[2]), result[3:]

    start = (jnp.zeros(weight_first.shape, jnp.float32), jnp.zeros(weight_second.shape, jnp.float32),
             jnp.zeros(weight_third.shape, jnp.float32))
    inputs = tuple(flatten(array) for array in (features, local_mask, halo_mask, boundary_index, labels, halo_first,
                                                halo_second, halo_third, return_second, return_third))
    sums, sends = lax.scan(advance, start, inputs)
    shaped = [route(piece.reshape((N_ROW, N_COL) + piece.shape[1:])) for piece in sends]
    return sums[0], sums[1], sums[2], shaped[0], shaped[1], shaped[2], shaped[3]
```

```python
import jax
import jax.numpy as jnp
from jax import lax
from jax.sharding import Mesh
from jax.sharding import PartitionSpec as P

ROW = ("row_0", "row_1")
COL = ("col_0", "col_1")


def slope(pre):
    sigma = jax.nn.sigmoid(pre)
    return sigma * (1.0 + pre * (1.0 - sigma))


def spread(local_bf, halo_bf, inverse, values, remote):
    summed = jnp.dot(local_bf, values, preferred_element_type=jnp.float32)
    summed = summed + values.astype(jnp.float32)
    summed = summed + jnp.dot(halo_bf, remote, preferred_element_type=jnp.float32)
    return (summed * inverse).astype(jnp.bfloat16)


def retract(local_bf, halo_bf, inverse, upstream, weight, hits, returned):
    across = jnp.dot(upstream, weight.T, preferred_element_type=jnp.float32)
    scaled = (across * inverse).astype(jnp.bfloat16)
    carried = jnp.dot(local_bf.T, scaled, preferred_element_type=jnp.float32) + scaled.astype(
        jnp.float32
    )
    carried = carried + jnp.dot(hits, returned, preferred_element_type=jnp.float32)
    outgoing = jnp.dot(halo_bf.T, scaled, preferred_element_type=jnp.float32).astype(jnp.bfloat16)
    return (carried, outgoing)


GROUP = ("row_1", "col_0", "col_1")
FAR = ("row_0",)
ROWS = 1024


def shares(axes):
    size = 1
    for axis in axes:
        size *= lax.axis_size(axis)
    return size


def copies(piece, axes):
    size = shares(axes)
    return lax.all_to_all(jnp.broadcast_to(piece[None], (size, *piece.shape)), axes, 0, 0, tiled=True)


def summed(pieces):
    return jnp.sum(pieces.astype(jnp.float32), axis=0).astype(jnp.bfloat16)


def total_of(packed):
    size = shares(GROUP)
    pieces = packed.reshape(size, packed.shape[0] // size, packed.shape[1])
    own = summed(lax.all_to_all(pieces, GROUP, 0, 0, tiled=True))
    own = summed(copies(own, FAR))
    return copies(own, GROUP).reshape(packed.shape)


def shifted(block, axis, step):
    size = lax.axis_size(axis)
    pairs = [(i, i + step) for i in range(size) if 0 <= i + step < size]
    return lax.ppermute(block, axis, pairs)


def traded(arrays):
    blocks = jnp.stack([a.reshape(4, a.shape[0] // 4, a.shape[1]) for a in arrays], axis=1)
    got = [
        shifted(blocks[1], ROW, 1),
        shifted(blocks[0], ROW, -1),
        shifted(blocks[3], COL, 1),
        shifted(blocks[2], COL, -1),
    ]
    return [jnp.concatenate([g[n] for g in got], axis=0)[None, None] for n in range(len(arrays))]


def per_device(
    features,
    local_mask,
    halo_mask,
    boundary_index,
    labels,
    halo_first,
    halo_second,
    halo_third,
    return_second,
    return_third,
    weight_first,
    weight_second,
    weight_third,
):
    features = features[0, 0]
    local_mask = local_mask[0, 0]
    halo_mask = halo_mask[0, 0]
    boundary_index = boundary_index[0, 0]
    labels = labels[0, 0]
    local_bf = local_mask.astype(jnp.bfloat16)
    halo_bf = halo_mask.astype(jnp.bfloat16)
    degree = (
        1.0
        + jnp.sum(local_mask, axis=1).astype(jnp.float32)
        + jnp.sum(halo_mask, axis=1).astype(jnp.float32)
    )
    inverse = (1.0 / degree)[:, None]
    node_rows = features.shape[0]
    hits = (jnp.arange(node_rows, dtype=jnp.int32)[:, None] == boundary_index[None, :]).astype(
        jnp.bfloat16
    )
    mixed_one = spread(local_bf, halo_bf, inverse, features, halo_first[0, 0])
    pre_one = jnp.dot(mixed_one, weight_first, preferred_element_type=jnp.float32)
    hidden_one = jax.nn.silu(pre_one).astype(jnp.bfloat16)
    mixed_two = spread(local_bf, halo_bf, inverse, hidden_one, halo_second[0, 0])
    pre_two = jnp.dot(mixed_two, weight_second, preferred_element_type=jnp.float32)
    hidden_two = jax.nn.silu(pre_two).astype(jnp.bfloat16)
    mixed_three = spread(local_bf, halo_bf, inverse, hidden_two, halo_third[0, 0])
    logits = jnp.dot(mixed_three, weight_third, preferred_element_type=jnp.float32)
    expo = jnp.exp(logits)
    probs = expo / jnp.sum(expo, axis=1, keepdims=True)
    target = (labels[:, None] == jnp.arange(logits.shape[1], dtype=jnp.int32)[None, :]).astype(
        jnp.float32
    )
    upstream_three = ((probs - target) / node_rows).astype(jnp.bfloat16)
    grad_three = jnp.dot(upstream_three.T, mixed_three, preferred_element_type=jnp.float32)
    carried_two, outgoing_three = retract(
        local_bf, halo_bf, inverse, upstream_three, weight_third, hits, return_third[0, 0]
    )
    upstream_two = (carried_two * slope(pre_two)).astype(jnp.bfloat16)
    grad_two = jnp.dot(mixed_two.T, upstream_two, preferred_element_type=jnp.float32)
    carried_one, outgoing_two = retract(
        local_bf, halo_bf, inverse, upstream_two, weight_second, hits, return_second[0, 0]
    )
    upstream_one = (carried_one * slope(pre_one)).astype(jnp.bfloat16)
    grad_one = jnp.dot(mixed_one.T, upstream_one, preferred_element_type=jnp.float32)
    hidden = jnp.concatenate([hidden_one, hidden_two], axis=1)
    sent = jnp.dot(hits.T, hidden, preferred_element_type=jnp.float32).astype(jnp.bfloat16)
    width = hidden_one.shape[1]
    next_second, next_third, back_second, back_third = traded(
        (sent[:, :width], sent[:, width:], outgoing_two, outgoing_three)
    )
    one, two, three = grad_one.shape[0], grad_two.shape[0], grad_three.shape[0]
    third_at = two + one + (-one) % 8
    packed = jnp.concatenate(
        [
            grad_two.astype(jnp.bfloat16),
            jnp.pad(grad_one.astype(jnp.bfloat16), [(0, (-one) % 8), (0, 0)]),
            jnp.pad(grad_three.astype(jnp.bfloat16), [(0, ROWS - third_at - three), (0, 0)]),
        ],
        axis=0,
    )
    total = total_of(packed).astype(jnp.float32)
    grad_two = total[:two]
    grad_one = total[two : two + one]
    grad_three = total[third_at : third_at + three].T
    return (grad_one, grad_two, grad_three, next_second, next_third, back_second, back_third)


def solution(mesh):
    torus = Mesh(mesh.devices.reshape(8, 2, 4, 4), ("row_0", "row_1", "col_0", "col_1"))
    in_specs = (
        P(ROW, COL, None, None),
        P(ROW, COL, None, None),
        P(ROW, COL, None, None),
        P(ROW, COL, None),
        P(ROW, COL, None),
        P(ROW, COL, None, None),
        P(ROW, COL, None, None),
        P(ROW, COL, None, None),
        P(ROW, COL, None, None),
        P(ROW, COL, None, None),
        P(),
        P(),
        P(),
    )
    out_specs = (
        P(),
        P(),
        P(),
        P(ROW, COL, None, None),
        P(ROW, COL, None, None),
        P(ROW, COL, None, None),
        P(ROW, COL, None, None),
    )
    return jax.shard_map(
        per_device, mesh=torus, in_specs=in_specs, out_specs=out_specs, check_vma=False
    )
```

```python
import jax
import jax.numpy as jnp
from jax import lax
from jax.experimental import pallas as pl
from jax.experimental.pallas import tpu as pltpu
from jax.sharding import Mesh
from jax.sharding import PartitionSpec as P

ROW = ("row_0", "row_1")
COL = ("col_0", "col_1")


def dot(a, b, contract=(1, 0)):
    dims = (((contract[0],), (contract[1],)), ((), ()))
    return lax.dot_general(a, b, dims, preferred_element_type=jnp.float32)


def silu_of(pre):
    return pre / (1.0 + jnp.exp(-pre))


def slope(pre):
    sigma = 1.0 / (1.0 + jnp.exp(-pre))
    return sigma * (1.0 + pre * (1.0 - sigma))


BF = jnp.bfloat16
F32 = jnp.float32
CHUNKS = 4
ROWS = 1024


def step_kernel(
    index_ref, label_ref, features, local_mask, halo_mask, halo_first, halo_second, halo_third,
    return_second, return_third, weight_first, weight_second, weight_third,
    packed_out, above_out, below_out, left_out, right_out,
    feat, local_raw, halo_raw, first, second, third, ret_two, ret_three, w_one, w_two, w_three,
    local, halo, hits, inverse, mixed_one, mixed_two, mixed_three, pre_one, pre_two,
    hidden_one, hidden_two, scaled, packed, sends, in_sem, local_sem, halo_sem, out_sem,
):
    nodes = feat.shape[0]
    rows = nodes // CHUNKS
    bound = hits.shape[1] // 4

    def fetch(source, target, sem):
        copy = pltpu.make_async_copy(source, target, sem)
        copy.start()
        return copy

    def part(ref, c):
        return ref.at[pl.ds(c * rows, rows)]

    got_feat = fetch(features, feat, in_sem.at[0])
    got_first = fetch(halo_first, first, in_sem.at[1])
    got_local, got_halo = [], []
    for c in range(CHUNKS):
        got_local.append(fetch(part(local_mask, c), part(local_raw, c), local_sem.at[c]))
        got_halo.append(fetch(part(halo_mask, c), part(halo_raw, c), halo_sem.at[c]))
    rest = [
        fetch(source, target, in_sem.at[2 + n])
        for n, (source, target) in enumerate(
            (
                (weight_first, w_one), (weight_second, w_two), (halo_second, second),
                (weight_third, w_three), (halo_third, third),
                (return_third, ret_three), (return_second, ret_two),
            )
        )
    ]
    got_w_one, got_w_two, got_second, got_w_three, got_third, got_ret_three, got_ret_two = rest

    hits[...] = (
        lax.broadcasted_iota(jnp.int32, hits.shape, 0) == index_ref[...]
    ).astype(F32).astype(BF)

    got_feat.wait()
    got_first.wait()
    for c in range(CHUNKS):
        at = pl.ds(c * rows, rows)
        got_local[c].wait()
        got_halo[c].wait()
        raw_local = local_raw[at, :].astype(F32)
        raw_halo = halo_raw[at, :].astype(F32)
        local[at, :] = raw_local.astype(BF)
        halo[at, :] = raw_halo.astype(BF)
        degree = (
            1.0 + jnp.sum(raw_local, axis=1, keepdims=True) + jnp.sum(raw_halo, axis=1, keepdims=True)
        )
        inverse[at, :] = 1.0 / degree
        summed = dot(local[at, :], feat[...]) + feat[at, :].astype(F32) + dot(halo[at, :], first[...])
        mixed_one[at, :] = (summed * inverse[at, :]).astype(BF)
        if c == 0:
            got_w_one.wait()
        pre = dot(mixed_one[at, :], w_one[...])
        pre_one[at, :] = pre
        hidden_one[at, :] = silu_of(pre).astype(BF)

    def spread(values, remote, mixed):
        for c in range(CHUNKS):
            at = pl.ds(c * rows, rows)
            summed = dot(local[at, :], values[...]) + values[at, :].astype(F32) + dot(halo[at, :], remote[...])
            mixed[at, :] = (summed * inverse[at, :]).astype(BF)

    got_w_two.wait()
    got_second.wait()
    spread(hidden_one, second, mixed_two)
    pre = dot(mixed_two[...], w_two[...])
    pre_two[...] = pre
    hidden_two[...] = silu_of(pre).astype(BF)

    got_w_three.wait()
    got_third.wait()
    spread(hidden_two, third, mixed_three)
    logits = dot(mixed_three[...], w_three[...])
    expo = jnp.exp(logits)
    probs = expo / jnp.sum(expo, axis=1, keepdims=True)
    wide = 128
    target = jnp.transpose(
        (lax.broadcasted_iota(jnp.int32, (wide, nodes), 0) == label_ref[...]).astype(F32)
    )[:, : logits.shape[1]]
    up_three = ((probs - target) / nodes).astype(BF)

    out_refs = (above_out, below_out, left_out, right_out)

    def place(array, n):
        for k in range(4):
            sends[k, n] = array[k * bound : (k + 1) * bound].astype(BF)

    def retract(up, weight, returned):
        scaled[...] = (dot(up, weight, (1, 1)) * inverse[...]).astype(BF)
        carried = dot(local[...], scaled[...], (0, 0)) + scaled[...].astype(F32)
        return carried + dot(hits[...], returned[...])

    got_ret_three.wait()
    got_ret_two.wait()
    two = w_two.shape[0]
    one = w_one.shape[0]
    three = w_three.shape[1]
    third_at = two + one + (-one) % 8
    packed[pl.ds(two + one // 16 * 16, ROWS - two - one // 16 * 16), :] = jnp.zeros(
        (ROWS - two - one // 16 * 16, packed.shape[1]), BF
    )
    packed[pl.ds(third_at, three), :] = dot(up_three, mixed_three[...], (0, 0)).astype(BF)
    carried = retract(up_three, w_three[...], ret_three)
    place(dot(halo[...], scaled[...], (0, 0)), 3)
    up_two = (carried * slope(pre_two[...])).astype(BF)
    packed[pl.ds(0, two), :] = dot(mixed_two[...], up_two, (0, 0)).astype(BF)
    carried = retract(up_two, w_two[...], ret_two)
    up_one = (carried * slope(pre_one[...])).astype(BF)
    packed[pl.ds(two, one), :] = dot(mixed_one[...], up_one, (0, 0)).astype(BF)
    out = [fetch(packed, packed_out, out_sem.at[4])]
    place(dot(halo[...], scaled[...], (0, 0)), 2)
    place(dot(hits[...], hidden_one[...], (0, 0)), 0)
    place(dot(hits[...], hidden_two[...], (0, 0)), 1)
    out += [fetch(sends.at[k], out_refs[k], out_sem.at[k]) for k in range(4)]
    for copy in out:
        copy.wait()


def step(index, labels, *arrays):
    (features, local_mask, halo_mask, halo_first, halo_second, halo_third,
     return_second, return_third, weight_first, weight_second, weight_third) = arrays
    nodes, wide = features.shape
    slots, hidden = halo_second.shape
    v = pltpu.VMEM
    scratch = [v(a.shape, a.dtype) for a in arrays]
    scratch += [
        v((nodes, nodes), BF), v((nodes, slots), BF), v((nodes, slots), BF), v((nodes, 1), F32),
        v((nodes, wide), BF), v((nodes, hidden), BF), v((nodes, hidden), BF),
        v((nodes, hidden), F32), v((nodes, hidden), F32),
        v((nodes, hidden), BF), v((nodes, hidden), BF), v((nodes, hidden), BF),
        v((ROWS, hidden), BF), v((4, 4, slots // 4, hidden), BF),
        pltpu.SemaphoreType.DMA((9,)), pltpu.SemaphoreType.DMA((CHUNKS,)),
        pltpu.SemaphoreType.DMA((CHUNKS,)), pltpu.SemaphoreType.DMA((5,)),
    ]
    block = jax.ShapeDtypeStruct((4, slots // 4, hidden), BF)
    return pl.pallas_call(
        step_kernel,
        out_shape=[jax.ShapeDtypeStruct((ROWS, hidden), BF)] + [block] * 4,
        in_specs=[pl.BlockSpec(memory_space=pltpu.VMEM)] * 2 + [pl.BlockSpec(memory_space=pl.ANY)] * len(arrays),
        out_specs=[pl.BlockSpec(memory_space=pl.ANY)] * 5,
        scratch_shapes=scratch,
        compiler_params=pltpu.CompilerParams(vmem_limit_bytes=50 * 2**20),
        cost_estimate=pl.CostEstimate(flops=8_000_000_000, bytes_accessed=12_000_000, transcendentals=1_000_000),
        name="step",
    )(index, labels, *arrays)


GROUP = ("row_1", "col_0", "col_1")
FAR = ("row_0",)


def shares(axes):
    size = 1
    for axis in axes:
        size *= lax.axis_size(axis)
    return size


def copies(piece, axes):
    size = shares(axes)
    return lax.all_to_all(jnp.broadcast_to(piece[None], (size, *piece.shape)), axes, 0, 0, tiled=True)


def summed(pieces):
    return jnp.sum(pieces.astype(jnp.float32), axis=0).astype(jnp.bfloat16)


def total_of(packed):
    size = shares(GROUP)
    pieces = packed.reshape(size, packed.shape[0] // size, packed.shape[1])
    own = summed(lax.all_to_all(pieces, GROUP, 0, 0, tiled=True))
    own = summed(copies(own, FAR))
    return copies(own, GROUP).reshape(packed.shape)


def shifted(block, axis, step):
    size = lax.axis_size(axis)
    pairs = [(i, i + step) for i in range(size) if 0 <= i + step < size]
    return lax.ppermute(block, axis, pairs)


def traded(above, below, left, right):
    got = [shifted(below, ROW, 1), shifted(above, ROW, -1), shifted(right, COL, 1), shifted(left, COL, -1)]
    return [jnp.concatenate([g[n] for g in got], axis=0)[None, None] for n in range(4)]


def per_device(
    features,
    local_mask,
    halo_mask,
    boundary_index,
    labels,
    halo_first,
    halo_second,
    halo_third,
    return_second,
    return_third,
    weight_first,
    weight_second,
    weight_third,
):
    packed, *blocks = step(
        boundary_index[0],
        labels[0],
        features[0, 0],
        local_mask[0, 0],
        halo_mask[0, 0],
        halo_first[0, 0],
        halo_second[0, 0],
        halo_third[0, 0],
        return_second[0, 0],
        return_third[0, 0],
        weight_first,
        weight_second,
        weight_third,
    )
    next_second, next_third, back_second, back_third = traded(*blocks)
    one, two, three = weight_first.shape[0], weight_second.shape[0], weight_third.shape[1]
    third_at = two + one + (-one) % 8
    total = total_of(packed).astype(jnp.float32)
    grad_two = total[:two]
    grad_one = total[two : two + one]
    grad_three = total[third_at : third_at + three].T
    return (grad_one, grad_two, grad_three, next_second, next_third, back_second, back_third)


def solution(mesh):
    torus = Mesh(mesh.devices.reshape(8, 2, 4, 4), ("row_0", "row_1", "col_0", "col_1"))
    in_specs = (
        P(ROW, COL, None, None),
        P(ROW, COL, None, None),
        P(ROW, COL, None, None),
        P(ROW, COL, None),
        P(ROW, COL, None),
        P(ROW, COL, None, None),
        P(ROW, COL, None, None),
        P(ROW, COL, None, None),
        P(ROW, COL, None, None),
        P(ROW, COL, None, None),
        P(),
        P(),
        P(),
    )
    out_specs = (
        P(),
        P(),
        P(),
        P(ROW, COL, None, None),
        P(ROW, COL, None, None),
        P(ROW, COL, None, None),
        P(ROW, COL, None, None),
    )
    return jax.shard_map(
        per_device, mesh=torus, in_specs=in_specs, out_specs=out_specs, check_vma=False
    )
```

```python
import jax
import jax.numpy as jnp
from jax import lax
from jax.experimental import pallas as pl
from jax.experimental.pallas import tpu as pltpu
from jax.sharding import Mesh
from jax.sharding import PartitionSpec as P


ROW = ("row_0", "row_1")
COL = ("col_0", "col_1")


def dot(a, b, contract=(1, 0)):
    dims = (((contract[0],), (contract[1],)), ((), ()))
    return lax.dot_general(a, b, dims, preferred_element_type=jnp.float32)


def silu_of(pre):
    return pre / (1.0 + jnp.exp(-pre))


def slope(pre):
    sigma = 1.0 / (1.0 + jnp.exp(-pre))
    return sigma * (1.0 + pre * (1.0 - sigma))


BF = jnp.bfloat16
F32 = jnp.float32
CHUNKS = 4
ROWS = 1024


def padded_up(size):
    return size + (-size) % 128


def step_kernel(
    index_ref, label_ref, features, local_mask, halo_mask, halo_first, halo_second, halo_third,
    return_second, return_third, weight_first, weight_second, weight_third,
    packed_out, above_out, below_out, left_out, right_out,
    feat_t, local_raw, halo_raw, first_t, second, third, ret_two, ret_three, w_one, w_two, w_three,
    local, halo, hits, inverse, mixed_one, mixed_two, mixed_three, pre_one, pre_two,
    hidden_one, hidden_two, scaled, packed, sends, feat, first, in_sem, local_sem, halo_sem, out_sem,
):
    nodes, wide = feat.shape
    rows = nodes // CHUNKS
    bound = hits.shape[1] // 4

    def fetch(source, target, sem):
        copy = pltpu.make_async_copy(source, target, sem)
        copy.start()
        return copy

    def part(ref, c):
        return ref.at[pl.ds(c * rows, rows)]

    got_feat = fetch(features, feat_t, in_sem.at[0])
    got_first = fetch(halo_first, first_t, in_sem.at[1])
    got_local, got_halo = [], []
    for c in range(CHUNKS):
        got_local.append(fetch(part(local_mask, c), part(local_raw, c), local_sem.at[c]))
        got_halo.append(fetch(part(halo_mask, c), part(halo_raw, c), halo_sem.at[c]))
    rest = [
        fetch(source, target, in_sem.at[2 + n])
        for n, (source, target) in enumerate(
            (
                (weight_first, w_one), (weight_second, w_two), (halo_second, second),
                (weight_third, w_three), (halo_third, third),
                (return_third, ret_three), (return_second, ret_two),
            )
        )
    ]
    got_w_one, got_w_two, got_second, got_w_three, got_third, got_ret_three, got_ret_two = rest

    hits[...] = (
        lax.broadcasted_iota(jnp.int32, hits.shape, 0) == index_ref[...]
    ).astype(F32).astype(BF)

    got_feat.wait()
    feat[...] = jnp.transpose(feat_t[...])
    got_first.wait()
    first[...] = jnp.transpose(first_t[...])
    for c in range(CHUNKS):
        at = pl.ds(c * rows, rows)
        got_local[c].wait()
        got_halo[c].wait()
        raw_local = local_raw[at, :].astype(F32)
        raw_halo = halo_raw[at, :].astype(F32)
        local[at, :] = raw_local.astype(BF)
        halo[at, :] = raw_halo.astype(BF)
        degree = (
            1.0 + jnp.sum(raw_local, axis=1, keepdims=True) + jnp.sum(raw_halo, axis=1, keepdims=True)
        )
        inverse[at, :] = 1.0 / degree
        summed = dot(local[at, :], feat[...]) + feat[at, :].astype(F32) + dot(halo[at, :], first[...])
        mixed_one[at, :] = (summed * inverse[at, :]).astype(BF)
        if c == 0:
            got_w_one.wait()
        pre = dot(mixed_one[at, :], w_one[...])
        pre_one[at, :] = pre
        hidden_one[at, :] = silu_of(pre).astype(BF)

    def spread(values, remote, mixed):
        for c in range(CHUNKS):
            at = pl.ds(c * rows, rows)
            summed = dot(local[at, :], values[...]) + values[at, :].astype(F32) + dot(halo[at, :], remote[...])
            mixed[at, :] = (summed * inverse[at, :]).astype(BF)

    got_w_two.wait()
    got_second.wait()
    spread(hidden_one, second, mixed_two)
    pre = dot(mixed_two[...], w_two[...])
    pre_two[...] = pre
    hidden_two[...] = silu_of(pre).astype(BF)

    got_w_three.wait()
    got_third.wait()
    spread(hidden_two, third, mixed_three)
    logits = dot(mixed_three[...], w_three[...], (1, 1))
    expo = jnp.exp(logits)
    probs = expo / jnp.sum(expo, axis=1, keepdims=True)
    target = jnp.transpose(
        (lax.broadcasted_iota(jnp.int32, (128, nodes), 0) == label_ref[...]).astype(F32)
    )[:, : logits.shape[1]]
    up_three = ((probs - target) / nodes).astype(BF)

    out_refs = (above_out, below_out, left_out, right_out)

    def place(array, n):
        for k in range(4):
            sends[k, n] = array[k * bound : (k + 1) * bound].astype(BF)

    def retract(across, returned):
        scaled[...] = (across * inverse[...]).astype(BF)
        carried = dot(local[...], scaled[...], (0, 0)) + scaled[...].astype(F32)
        return carried + dot(hits[...], returned[...])

    got_ret_three.wait()
    got_ret_two.wait()
    two = w_two.shape[0]
    three = w_three.shape[0]
    third_at = two + padded_up(wide)
    tail = two + wide // 16 * 16
    packed[pl.ds(tail, ROWS - tail), :] = jnp.zeros((ROWS - tail, packed.shape[1]), BF)
    packed[pl.ds(third_at, three), :] = dot(up_three, mixed_three[...], (0, 0)).astype(BF)
    carried = retract(dot(up_three, w_three[...]), ret_three)
    place(dot(halo[...], scaled[...], (0, 0)), 3)
    up_two = (carried * slope(pre_two[...])).astype(BF)
    packed[pl.ds(0, two), :] = dot(mixed_two[...], up_two, (0, 0)).astype(BF)
    carried = retract(dot(up_two, w_two[...], (1, 1)), ret_two)
    up_one = (carried * slope(pre_one[...])).astype(BF)
    packed[pl.ds(two, wide), :] = dot(mixed_one[...], up_one, (0, 0)).astype(BF)
    out = [fetch(packed, packed_out, out_sem.at[4])]
    place(dot(halo[...], scaled[...], (0, 0)), 2)
    place(dot(hits[...], hidden_one[...], (0, 0)), 0)
    place(dot(hits[...], hidden_two[...], (0, 0)), 1)
    out += [fetch(sends.at[k], out_refs[k], out_sem.at[k]) for k in range(4)]
    for copy in out:
        copy.wait()


def step(index, labels, *arrays):
    (features, _, _, _, halo_second, _,
     _, _, _, _, _) = arrays
    depth, nodes = features.shape
    wide = depth
    slots, hidden = halo_second.shape
    v = pltpu.VMEM
    scratch = [v(a.shape, a.dtype) for a in arrays]
    scratch += [
        v((nodes, nodes), BF), v((nodes, slots), BF), v((nodes, slots), BF), v((nodes, 1), F32),
        v((nodes, wide), BF), v((nodes, hidden), BF), v((nodes, hidden), BF),
        v((nodes, hidden), F32), v((nodes, hidden), F32),
        v((nodes, hidden), BF), v((nodes, hidden), BF), v((nodes, hidden), BF),
        v((ROWS, hidden), BF), v((4, 4, slots // 4, hidden), BF),
        v((nodes, wide), BF), v((slots, wide), BF),
        pltpu.SemaphoreType.DMA((9,)), pltpu.SemaphoreType.DMA((CHUNKS,)),
        pltpu.SemaphoreType.DMA((CHUNKS,)), pltpu.SemaphoreType.DMA((5,)),
    ]
    block = jax.ShapeDtypeStruct((4, slots // 4, hidden), BF)
    return pl.pallas_call(
        step_kernel,
        out_shape=[jax.ShapeDtypeStruct((ROWS, hidden), BF)] + [block] * 4,
        in_specs=[pl.BlockSpec(memory_space=pltpu.VMEM)] * 2 + [pl.BlockSpec(memory_space=pltpu.HBM)] * len(arrays),
        out_specs=[pl.BlockSpec(memory_space=pl.ANY)] * 5,
        scratch_shapes=scratch,
        compiler_params=pltpu.CompilerParams(vmem_limit_bytes=66_000_000),
        cost_estimate=pl.CostEstimate(flops=8_000_000_000, bytes_accessed=12_000_000, transcendentals=1_000_000),
        name="step",
    )(index, labels, *arrays)


GROUP = ("row_1", "col_0", "col_1")
FAR = ("row_0",)


def shares(axes):
    size = 1
    for axis in axes:
        size *= lax.axis_size(axis)
    return size


def copies(piece, axes):
    size = shares(axes)
    return lax.all_to_all(jnp.broadcast_to(piece[None], (size, *piece.shape)), axes, 0, 0, tiled=True)


def summed(pieces):
    return jnp.sum(pieces.astype(jnp.float32), axis=0).astype(jnp.bfloat16)


def total_of(packed, lateral, vertical):
    size = shares(GROUP)
    pieces = packed.reshape(size, packed.shape[0] // size, packed.shape[1])
    own = lax.all_to_all(pieces, GROUP, 0, 0, tiled=True)
    first = lateral()
    own = summed(own)
    own = copies(own, FAR)
    own = summed(own)
    whole = copies(own, GROUP)
    last = vertical()
    return whole.reshape(packed.shape), first, last


def shifted(block, axis, step):
    size = lax.axis_size(axis)
    pairs = [(i, i + step) for i in range(size) if 0 <= i + step < size]
    return lax.ppermute(block, axis, pairs)


def per_device(
    features,
    local_mask,
    halo_mask,
    boundary_index,
    labels,
    halo_first,
    halo_second,
    halo_third,
    return_second,
    return_third,
    weight_first,
    weight_second,
    weight_third,
):
    packed, *blocks = step(
        boundary_index[0],
        labels[0],
        features[0, 0].T,
        local_mask[0, 0],
        halo_mask[0, 0],
        halo_first[0, 0].T,
        halo_second[0, 0],
        halo_third[0, 0],
        return_second[0, 0],
        return_third[0, 0],
        weight_first,
        weight_second,
        weight_third.T,
    )
    above, below, left, right = blocks

    def lateral():
        return [shifted(right, COL, 1), shifted(left, COL, -1)]

    def vertical():
        return [shifted(below, ROW, 1), shifted(above, ROW, -1)]

    one, two, three = weight_first.shape[0], weight_second.shape[0], weight_third.shape[1]
    third_at = two + padded_up(one)
    total, lateral_got, vertical_got = total_of(packed, lateral, vertical)
    got = vertical_got + lateral_got
    next_second, next_third, back_second, back_third = [
        jnp.concatenate([g[n] for g in got], axis=0)[None, None] for n in range(4)
    ]
    total = total.astype(jnp.float32)
    grad_two = total[:two]
    grad_one = total[two : two + one]
    grad_three = total[third_at : third_at + three].T
    return (grad_one, grad_two, grad_three, next_second, next_third, back_second, back_third)


def solution(mesh):
    torus = Mesh(mesh.devices.reshape(8, 2, 4, 4), ("row_0", "row_1", "col_0", "col_1"))
    in_specs = (
        P(ROW, COL, None, None),
        P(ROW, COL, None, None),
        P(ROW, COL, None, None),
        P(ROW, COL, None),
        P(ROW, COL, None),
        P(ROW, COL, None, None),
        P(ROW, COL, None, None),
        P(ROW, COL, None, None),
        P(ROW, COL, None, None),
        P(ROW, COL, None, None),
        P(),
        P(),
        P(),
    )
    out_specs = (
        P(),
        P(),
        P(),
        P(ROW, COL, None, None),
        P(ROW, COL, None, None),
        P(ROW, COL, None, None),
        P(ROW, COL, None, None),
    )
    return jax.shard_map(
        per_device, mesh=torus, in_specs=in_specs, out_specs=out_specs, check_vma=False
    )
```

```python
import jax
import jax.numpy as jnp
from jax import lax
from jax.experimental import pallas as pl
from jax.experimental.pallas import tpu as pltpu
from jax.sharding import Mesh
from jax.sharding import PartitionSpec as P


ROW = ("row_0", "row_1")
COL = ("col_0", "col_1")


def dot(a, b, contract=(1, 0)):
    dims = (((contract[0],), (contract[1],)), ((), ()))
    return lax.dot_general(a, b, dims, preferred_element_type=jnp.float32)


def silu_of(pre):
    return pre / (1.0 + jnp.exp(-pre))


def slope(pre):
    sigma = 1.0 / (1.0 + jnp.exp(-pre))
    return sigma * (1.0 + pre * (1.0 - sigma))


BF = jnp.bfloat16
F32 = jnp.float32
CHUNKS = 4
ROWS = 1024


def padded_up(size):
    return size + (-size) % 128


def step_kernel(
    core_ref, index_ref, label_ref, features, local_mask, halo_mask, halo_first, halo_second, halo_third,
    return_second, return_third, weight_first, weight_second, weight_third,
    keep_out, send_out, above_out, below_out, left_out, right_out,
    feat_t, local_raw, halo_raw, first_t, second, third, ret_two, ret_three, w_one, w_two, w_three,
    local, halo, hits, inverse, mixed_one, mixed_two, mixed_three, pre_one, pre_two,
    hidden_one, hidden_two, scaled, packed, sends, feat, first, in_sem, local_sem, halo_sem, out_sem,
):
    nodes, wide = feat.shape
    rows = nodes // CHUNKS
    bound = hits.shape[1] // 4

    def fetch(source, target, sem):
        copy = pltpu.make_async_copy(source, target, sem)
        copy.start()
        return copy

    def part(ref, c):
        return ref.at[pl.ds(c * rows, rows)]

    got_feat = fetch(features, feat_t, in_sem.at[0])
    got_first = fetch(halo_first, first_t, in_sem.at[1])
    got_local, got_halo = [], []
    for c in range(CHUNKS):
        got_local.append(fetch(part(local_mask, c), part(local_raw, c), local_sem.at[c]))
        got_halo.append(fetch(part(halo_mask, c), part(halo_raw, c), halo_sem.at[c]))
    rest = [
        fetch(source, target, in_sem.at[2 + n])
        for n, (source, target) in enumerate(
            (
                (weight_first, w_one), (weight_second, w_two), (halo_second, second),
                (weight_third, w_three), (halo_third, third),
                (return_third, ret_three), (return_second, ret_two),
            )
        )
    ]
    got_w_one, got_w_two, got_second, got_w_three, got_third, got_ret_three, got_ret_two = rest

    hits[...] = (
        lax.broadcasted_iota(jnp.int32, hits.shape, 0) == index_ref[...]
    ).astype(F32).astype(BF)

    got_feat.wait()
    feat[...] = jnp.transpose(feat_t[...])
    got_first.wait()
    first[...] = jnp.transpose(first_t[...])
    for c in range(CHUNKS):
        at = pl.ds(c * rows, rows)
        got_local[c].wait()
        got_halo[c].wait()
        raw_local = local_raw[at, :].astype(F32)
        raw_halo = halo_raw[at, :].astype(F32)
        local[at, :] = raw_local.astype(BF)
        halo[at, :] = raw_halo.astype(BF)
        degree = (
            1.0 + jnp.sum(raw_local, axis=1, keepdims=True) + jnp.sum(raw_halo, axis=1, keepdims=True)
        )
        inverse[at, :] = 1.0 / degree
        summed = dot(local[at, :], feat[...]) + feat[at, :].astype(F32) + dot(halo[at, :], first[...])
        mixed_one[at, :] = (summed * inverse[at, :]).astype(BF)
        if c == 0:
            got_w_one.wait()
        pre = dot(mixed_one[at, :], w_one[...])
        pre_one[at, :] = pre
        hidden_one[at, :] = silu_of(pre).astype(BF)

    def spread(values, remote, mixed):
        for c in range(CHUNKS):
            at = pl.ds(c * rows, rows)
            summed = dot(local[at, :], values[...]) + values[at, :].astype(F32) + dot(halo[at, :], remote[...])
            mixed[at, :] = (summed * inverse[at, :]).astype(BF)

    got_w_two.wait()
    got_second.wait()
    spread(hidden_one, second, mixed_two)
    pre = dot(mixed_two[...], w_two[...])
    pre_two[...] = pre
    hidden_two[...] = silu_of(pre).astype(BF)

    got_w_three.wait()
    got_third.wait()
    spread(hidden_two, third, mixed_three)
    logits = dot(mixed_three[...], w_three[...], (1, 1))
    expo = jnp.exp(logits)
    probs = expo / jnp.sum(expo, axis=1, keepdims=True)
    target = jnp.transpose(
        (lax.broadcasted_iota(jnp.int32, (128, nodes), 0) == label_ref[...]).astype(F32)
    )[:, : logits.shape[1]]
    up_three = ((probs - target) / nodes).astype(BF)

    out_refs = (above_out, below_out, left_out, right_out)

    def place(array, n):
        for k in range(4):
            sends[k, n] = array[k * bound : (k + 1) * bound].astype(BF)

    def retract(across, returned):
        scaled[...] = (across * inverse[...]).astype(BF)
        carried = dot(local[...], scaled[...], (0, 0)) + scaled[...].astype(F32)
        return carried + dot(hits[...], returned[...])

    got_ret_three.wait()
    got_ret_two.wait()
    two = w_two.shape[0]
    third_at = two + padded_up(wide)
    tail = two + wide // 16 * 16
    half = packed.shape[2]
    for h in range(2):
        packed[h, pl.ds(tail, ROWS - tail), :] = jnp.zeros((ROWS - tail, half), BF)

    def pack(row, grad):
        for h in range(2):
            packed[h, pl.ds(row, grad.shape[0]), :] = grad[:, h * half : (h + 1) * half].astype(BF)

    pack(third_at, dot(up_three, mixed_three[...], (0, 0)))
    carried = retract(dot(up_three, w_three[...]), ret_three)
    place(dot(halo[...], scaled[...], (0, 0)), 3)
    up_two = (carried * slope(pre_two[...])).astype(BF)
    pack(0, dot(mixed_two[...], up_two, (0, 0)))
    carried = retract(dot(up_two, w_two[...], (1, 1)), ret_two)
    up_one = (carried * slope(pre_one[...])).astype(BF)
    pack(two, dot(mixed_one[...], up_one, (0, 0)))
    core = core_ref[0]
    out = [fetch(packed.at[1 - core], send_out, out_sem.at[4]), fetch(packed.at[core], keep_out, out_sem.at[5])]
    place(dot(halo[...], scaled[...], (0, 0)), 2)
    place(dot(hits[...], hidden_one[...], (0, 0)), 0)
    place(dot(hits[...], hidden_two[...], (0, 0)), 1)
    out += [fetch(sends.at[k], out_refs[k], out_sem.at[k]) for k in range(4)]
    for copy in out:
        copy.wait()


def step(core, index, labels, *arrays):
    (features, _, _, _, halo_second, _,
     _, _, _, _, _) = arrays
    depth, nodes = features.shape
    wide = depth
    slots, hidden = halo_second.shape
    v = pltpu.VMEM
    scratch = [v(a.shape, a.dtype) for a in arrays]
    scratch += [
        v((nodes, nodes), BF), v((nodes, slots), BF), v((nodes, slots), BF), v((nodes, 1), F32),
        v((nodes, wide), BF), v((nodes, hidden), BF), v((nodes, hidden), BF),
        v((nodes, hidden), F32), v((nodes, hidden), F32),
        v((nodes, hidden), BF), v((nodes, hidden), BF), v((nodes, hidden), BF),
        v((2, ROWS, hidden // 2), BF), v((4, 4, slots // 4, hidden), BF),
        v((nodes, wide), BF), v((slots, wide), BF),
        pltpu.SemaphoreType.DMA((9,)), pltpu.SemaphoreType.DMA((CHUNKS,)),
        pltpu.SemaphoreType.DMA((CHUNKS,)), pltpu.SemaphoreType.DMA((6,)),
    ]
    block = v((4, slots // 4, hidden), BF)
    return pl.pallas_call(
        step_kernel,
        out_shape=[pltpu.VMEM((ROWS, hidden // 2), BF)] * 2 + [block] * 4,
        in_specs=[pl.BlockSpec(memory_space=pltpu.SMEM)]
        + [pl.BlockSpec(memory_space=pltpu.VMEM)] * 2
        + [pl.BlockSpec(memory_space=pltpu.HBM)] * len(arrays),
        out_specs=[pl.BlockSpec(memory_space=pl.ANY)] * 6,
        scratch_shapes=scratch,
        compiler_params=pltpu.CompilerParams(vmem_limit_bytes=62_000_000),
        cost_estimate=pl.CostEstimate(flops=8_000_000_000, bytes_accessed=12_000_000, transcendentals=1_000_000),
        name="step",
    )(core, index, labels, *arrays)


def unpack_kernel(core_ref, mine, other, one_out, two_out, three_out):
    own_left = core_ref[0] == 0
    half = mine.shape[1]

    def rows_of(row, count):
        a, b = mine[pl.ds(row, count), :].astype(F32), other[pl.ds(row, count), :].astype(F32)
        return jnp.where(own_left, a, b), jnp.where(own_left, b, a)

    row = 0
    for out in (two_out, one_out, three_out):
        for h, part in enumerate(rows_of(row, out.shape[0])):
            out[:, h * half : (h + 1) * half] = part
        row += out.shape[0] if out is two_out else padded_up(out.shape[0])


def unpack(core, mine, other, one, two, three):
    wide = mine.shape[1] * 2
    return pl.pallas_call(
        unpack_kernel,
        out_shape=[jax.ShapeDtypeStruct((n, wide), F32) for n in (one, two, three)],
        in_specs=[pl.BlockSpec(memory_space=pltpu.SMEM)] + [pl.BlockSpec(memory_space=pltpu.VMEM)] * 2,
        out_specs=[pl.BlockSpec(memory_space=pltpu.VMEM)] * 3,
        cost_estimate=pl.CostEstimate(flops=1_000_000, bytes_accessed=1_500_000, transcendentals=0),
        compiler_params=pltpu.CompilerParams(vmem_limit_bytes=8 * 2**20),
        name="unpack",
    )(core, mine, other)


PAIR = "row_1"
GROUP = COL
FAR = ("row_0",)


def shares(axes):
    size = 1
    for axis in axes:
        size *= lax.axis_size(axis)
    return size


def copies(piece, axes):
    size = shares(axes)
    return lax.all_to_all(jnp.broadcast_to(piece[None], (size, *piece.shape)), axes, 0, 0, tiled=True)


def summed(pieces):
    return jnp.sum(pieces.astype(jnp.float32), axis=0).astype(jnp.bfloat16)


def swapped(half):
    return lax.ppermute(half, PAIR, [(0, 1), (1, 0)])


def joined(got):
    return [jnp.concatenate([g[n] for g in got], axis=0)[None, None] for n in range(4)]


def total_of(keep, send, beside_in, beside_far):
    size = shares(GROUP)
    other = swapped(send)
    own = (keep.astype(F32) + other.astype(F32)).astype(BF)
    pieces = own.reshape(size, own.shape[0] // size, own.shape[1])
    own = lax.all_to_all(pieces, GROUP, 0, 0, tiled=True)
    first = beside_in()
    own = summed(own)
    own = copies(own, FAR)
    last = beside_far()
    own = summed(own)
    mine = copies(own, GROUP).reshape(keep.shape)
    mine, *outs = lax.optimization_barrier((mine, *joined(first + last)))
    other = swapped(mine)
    return mine, other, outs


def shifted(block, axis, step):
    size = lax.axis_size(axis)
    pairs = [(i, i + step) for i in range(size) if 0 <= i + step < size]
    return lax.ppermute(block, axis, pairs)


def per_device(
    features,
    local_mask,
    halo_mask,
    boundary_index,
    labels,
    halo_first,
    halo_second,
    halo_third,
    return_second,
    return_third,
    weight_first,
    weight_second,
    weight_third,
):
    core = lax.axis_index(PAIR).astype(jnp.int32).reshape(1)
    keep, send, *blocks = step(
        core,
        boundary_index[0],
        labels[0],
        features[0, 0].T,
        local_mask[0, 0],
        halo_mask[0, 0],
        halo_first[0, 0].T,
        halo_second[0, 0],
        halo_third[0, 0],
        return_second[0, 0],
        return_third[0, 0],
        weight_first,
        weight_second,
        weight_third.T,
    )
    above, below, left, right = blocks

    def beside_in():
        return [shifted(below, ROW, 1), shifted(above, ROW, -1), shifted(right, COL, 1)]

    def beside_far():
        return [shifted(left, COL, -1)]

    one, two, three = weight_first.shape[0], weight_second.shape[0], weight_third.shape[1]
    mine, other, outs = total_of(keep, send, beside_in, beside_far)
    next_second, next_third, back_second, back_third = outs
    grad_one, grad_two, grad_three = unpack(core, mine, other, one, two, three)
    grad_three = grad_three.T
    return (grad_one, grad_two, grad_three, next_second, next_third, back_second, back_third)


def solution(mesh):
    torus = Mesh(mesh.devices.reshape(8, 2, 4, 4), ("row_0", "row_1", "col_0", "col_1"))
    in_specs = (
        P(ROW, COL, None, None),
        P(ROW, COL, None, None),
        P(ROW, COL, None, None),
        P(ROW, COL, None),
        P(ROW, COL, None),
        P(ROW, COL, None, None),
        P(ROW, COL, None, None),
        P(ROW, COL, None, None),
        P(ROW, COL, None, None),
        P(ROW, COL, None, None),
        P(),
        P(),
        P(),
    )
    out_specs = (
        P(),
        P(),
        P(),
        P(ROW, COL, None, None),
        P(ROW, COL, None, None),
        P(ROW, COL, None, None),
        P(ROW, COL, None, None),
    )
    return jax.shard_map(
        per_device, mesh=torus, in_specs=in_specs, out_specs=out_specs, check_vma=False
    )
```

```python
import jax
import jax.numpy as jnp
from jax import lax
from jax.experimental import pallas as pl
from jax.experimental.pallas import tpu as pltpu
from jax.sharding import Mesh
from jax.sharding import PartitionSpec as P


ROW = ("row_0", "row_1")
COL = ("col_0", "col_1")


def dot(a, b, contract=(1, 0)):
    dims = (((contract[0],), (contract[1],)), ((), ()))
    return lax.dot_general(a, b, dims, preferred_element_type=jnp.float32)


def silu_of(pre):
    return pre / (1.0 + jnp.exp(-pre))


def slope(pre):
    sigma = 1.0 / (1.0 + jnp.exp(-pre))
    return sigma * (1.0 + pre * (1.0 - sigma))


BF = jnp.bfloat16
F32 = jnp.float32
CHUNKS = 4
ROWS = 1024


def padded_up(size):
    return size + (-size) % 128


def step_kernel(
    core_ref, index_ref, label_ref, features, local_mask, halo_mask, halo_first, halo_second, halo_third,
    return_second, return_third, weight_first, weight_second, weight_third,
    keep_out, pair_out, far_out, left_out, right_out,
    feat_t, local_raw, halo_raw, first_t, second, third, ret_two, ret_three, w_one, w_two, w_three,
    local, halo, hits, inverse, mixed_one, mixed_two, mixed_three, pre_one, pre_two,
    hidden_one, hidden_two, scaled, packed, upright, sends, feat, first, in_sem, local_sem, halo_sem, out_sem,
):
    nodes, wide = feat.shape
    rows = nodes // CHUNKS
    bound = hits.shape[1] // 4

    def fetch(source, target, sem):
        copy = pltpu.make_async_copy(source, target, sem)
        copy.start()
        return copy

    def part(ref, c):
        return ref.at[pl.ds(c * rows, rows)]

    got_feat = fetch(features, feat_t, in_sem.at[0])
    got_first = fetch(halo_first, first_t, in_sem.at[1])
    got_local, got_halo = [], []
    for c in range(CHUNKS):
        got_local.append(fetch(part(local_mask, c), part(local_raw, c), local_sem.at[c]))
        got_halo.append(fetch(part(halo_mask, c), part(halo_raw, c), halo_sem.at[c]))
    rest = [
        fetch(source, target, in_sem.at[2 + n])
        for n, (source, target) in enumerate(
            (
                (weight_first, w_one), (weight_second, w_two), (halo_second, second),
                (weight_third, w_three), (halo_third, third),
                (return_third, ret_three), (return_second, ret_two),
            )
        )
    ]
    got_w_one, got_w_two, got_second, got_w_three, got_third, got_ret_three, got_ret_two = rest

    hits[...] = (
        lax.broadcasted_iota(jnp.int32, hits.shape, 0) == index_ref[...]
    ).astype(F32).astype(BF)

    got_feat.wait()
    feat[...] = jnp.transpose(feat_t[...])
    got_first.wait()
    first[...] = jnp.transpose(first_t[...])
    for c in range(CHUNKS):
        at = pl.ds(c * rows, rows)
        got_local[c].wait()
        got_halo[c].wait()
        raw_local = local_raw[at, :].astype(F32)
        raw_halo = halo_raw[at, :].astype(F32)
        local[at, :] = raw_local.astype(BF)
        halo[at, :] = raw_halo.astype(BF)
        degree = (
            1.0 + jnp.sum(raw_local, axis=1, keepdims=True) + jnp.sum(raw_halo, axis=1, keepdims=True)
        )
        inverse[at, :] = 1.0 / degree
        summed = dot(local[at, :], feat[...]) + feat[at, :].astype(F32) + dot(halo[at, :], first[...])
        mixed_one[at, :] = (summed * inverse[at, :]).astype(BF)
        if c == 0:
            got_w_one.wait()
        pre = dot(mixed_one[at, :], w_one[...])
        pre_one[at, :] = pre
        hidden_one[at, :] = silu_of(pre).astype(BF)

    def spread(values, remote, mixed):
        for c in range(CHUNKS):
            at = pl.ds(c * rows, rows)
            summed = dot(local[at, :], values[...]) + values[at, :].astype(F32) + dot(halo[at, :], remote[...])
            mixed[at, :] = (summed * inverse[at, :]).astype(BF)

    got_w_two.wait()
    got_second.wait()
    spread(hidden_one, second, mixed_two)
    pre = dot(mixed_two[...], w_two[...])
    pre_two[...] = pre
    hidden_two[...] = silu_of(pre).astype(BF)

    got_w_three.wait()
    got_third.wait()
    spread(hidden_two, third, mixed_three)
    logits = dot(mixed_three[...], w_three[...], (1, 1))
    expo = jnp.exp(logits)
    probs = expo / jnp.sum(expo, axis=1, keepdims=True)
    target = jnp.transpose(
        (lax.broadcasted_iota(jnp.int32, (128, nodes), 0) == label_ref[...]).astype(F32)
    )[:, : logits.shape[1]]
    up_three = ((probs - target) / nodes).astype(BF)

    half = packed.shape[2]

    def place(array, n):
        for k in range(2):
            for h in range(2):
                upright[k, pl.ds((2 * n + h) * bound, bound), :] = array[
                    k * bound : (k + 1) * bound, h * half : (h + 1) * half
                ].astype(BF)
            sends[k, n] = array[(2 + k) * bound : (3 + k) * bound].astype(BF)

    def retract(across, returned):
        scaled[...] = (across * inverse[...]).astype(BF)
        carried = dot(local[...], scaled[...], (0, 0)) + scaled[...].astype(F32)
        return carried + dot(hits[...], returned[...])

    got_ret_three.wait()
    got_ret_two.wait()
    two = w_two.shape[0]
    third_at = two + padded_up(wide)
    tail = two + wide // 16 * 16
    for h in range(2):
        packed[h, pl.ds(tail, ROWS - tail), :] = jnp.zeros((ROWS - tail, half), BF)

    def pack(row, grad):
        for h in range(2):
            packed[h, pl.ds(row, grad.shape[0]), :] = grad[:, h * half : (h + 1) * half].astype(BF)

    pack(third_at, dot(up_three, mixed_three[...], (0, 0)))
    carried = retract(dot(up_three, w_three[...]), ret_three)
    place(dot(halo[...], scaled[...], (0, 0)), 3)
    up_two = (carried * slope(pre_two[...])).astype(BF)
    pack(0, dot(mixed_two[...], up_two, (0, 0)))
    carried = retract(dot(up_two, w_two[...], (1, 1)), ret_two)
    up_one = (carried * slope(pre_one[...])).astype(BF)
    pack(two, dot(mixed_one[...], up_one, (0, 0)))
    core = core_ref[0]
    out = [fetch(packed.at[1 - core], pair_out.at[0], out_sem.at[4]), fetch(packed.at[core], keep_out, out_sem.at[5])]
    place(dot(halo[...], scaled[...], (0, 0)), 2)
    place(dot(hits[...], hidden_one[...], (0, 0)), 0)
    place(dot(hits[...], hidden_two[...], (0, 0)), 1)
    out += [
        fetch(upright.at[1 - core], pair_out.at[1], out_sem.at[0]),
        fetch(upright.at[core], far_out, out_sem.at[1]),
        fetch(sends.at[0], left_out, out_sem.at[2]),
        fetch(sends.at[1], right_out, out_sem.at[3]),
    ]
    for copy in out:
        copy.wait()


def step(core, index, labels, *arrays):
    (features, _, _, _, halo_second, _,
     _, _, _, _, _) = arrays
    depth, nodes = features.shape
    wide = depth
    slots, hidden = halo_second.shape
    v = pltpu.VMEM
    scratch = [v(a.shape, a.dtype) for a in arrays]
    scratch += [
        v((nodes, nodes), BF), v((nodes, slots), BF), v((nodes, slots), BF), v((nodes, 1), F32),
        v((nodes, wide), BF), v((nodes, hidden), BF), v((nodes, hidden), BF),
        v((nodes, hidden), F32), v((nodes, hidden), F32),
        v((nodes, hidden), BF), v((nodes, hidden), BF), v((nodes, hidden), BF),
        v((2, ROWS, hidden // 2), BF), v((2, 2 * slots, hidden // 2), BF),
        v((2, 4, slots // 4, hidden), BF),
        v((nodes, wide), BF), v((slots, wide), BF),
        pltpu.SemaphoreType.DMA((9,)), pltpu.SemaphoreType.DMA((CHUNKS,)),
        pltpu.SemaphoreType.DMA((CHUNKS,)), pltpu.SemaphoreType.DMA((6,)),
    ]
    half = v((ROWS, hidden // 2), BF)
    block = v((4, slots // 4, hidden), BF)
    return pl.pallas_call(
        step_kernel,
        out_shape=[half, v((2, ROWS, hidden // 2), BF), half, block, block],
        in_specs=[pl.BlockSpec(memory_space=pltpu.SMEM)]
        + [pl.BlockSpec(memory_space=pltpu.VMEM)] * 2
        + [pl.BlockSpec(memory_space=pltpu.HBM)] * len(arrays),
        out_specs=[pl.BlockSpec(memory_space=pl.ANY)] * 5,
        scratch_shapes=scratch,
        compiler_params=pltpu.CompilerParams(vmem_limit_bytes=62_000_000),
        cost_estimate=pl.CostEstimate(flops=8_000_000_000, bytes_accessed=12_000_000, transcendentals=1_000_000),
        name="step",
    )(core, index, labels, *arrays)


def small(kernel, out_shape, *arrays):
    scalars = sum(a.ndim == 1 for a in arrays)
    return pl.pallas_call(
        kernel,
        out_shape=out_shape,
        in_specs=[pl.BlockSpec(memory_space=pltpu.SMEM)] * scalars
        + [pl.BlockSpec(memory_space=pltpu.VMEM)] * (len(arrays) - scalars),
        out_specs=jax.tree.map(lambda _: pl.BlockSpec(memory_space=pltpu.VMEM), out_shape),
        compiler_params=pltpu.CompilerParams(vmem_limit_bytes=8 * 2**20),
        cost_estimate=pl.CostEstimate(flops=500_000, bytes_accessed=1_000_000, transcendentals=0),
    )(*arrays)


def add_kernel(keep, pair, out):
    out[...] = (keep[...].astype(F32) + pair[0].astype(F32)).astype(BF)


def sum_kernel(pieces, out):
    total = pieces[0].astype(F32)
    for n in range(1, pieces.shape[0]):
        total = total + pieces[n].astype(F32)
    total = total.astype(BF)
    for n in range(out.shape[0]):
        out[n] = total


def repeated_sum(pieces, count):
    return small(sum_kernel, pltpu.VMEM((count, *pieces.shape[1:]), BF), pieces)


def join_kernel(core_ref, pair, far, right, left, *outs):
    upper = core_ref[0] == 0
    bound, half = right.shape[1], pair.shape[2]
    for n, out in enumerate(outs):
        for h in range(2):
            at = pl.ds((2 * n + h) * bound, bound)
            cols = slice(h * half, (h + 1) * half)
            near, away = pair[1, at, :], far[at, :]
            out[0:bound, cols] = jnp.where(upper, away, near)
            out[bound : 2 * bound, cols] = jnp.where(upper, near, away)
        out[2 * bound : 3 * bound, :] = right[n]
        out[3 * bound : 4 * bound, :] = left[n]


def unpack_kernel(core_ref, mine, other, one_out, two_out, three_out):
    own_left = core_ref[0] == 0
    half = mine.shape[1]

    def rows_of(row, count):
        a, b = mine[pl.ds(row, count), :].astype(F32), other[pl.ds(row, count), :].astype(F32)
        return jnp.where(own_left, a, b), jnp.where(own_left, b, a)

    row = 0
    for out in (two_out, one_out, three_out):
        for h, part in enumerate(rows_of(row, out.shape[0])):
            out[:, h * half : (h + 1) * half] = part
        row += out.shape[0] if out is two_out else padded_up(out.shape[0])


def unpack(core, mine, other, one, two, three):
    wide = mine.shape[1] * 2
    shapes = [jax.ShapeDtypeStruct((n, wide), F32) for n in (one, two, three)]
    return small(unpack_kernel, shapes, core, mine, other)


PAIR = "row_1"
GROUP = COL
FAR = ("row_0",)


def shares(axes):
    size = 1
    for axis in axes:
        size *= lax.axis_size(axis)
    return size


def exchanged(pieces, axes):
    return lax.all_to_all(pieces, axes, 0, 0, tiled=True)


def swapped(half):
    return lax.ppermute(half, PAIR, [(0, 1), (1, 0)])


def total_of(core, keep, pair, beside_in, beside_far):
    size = shares(GROUP)
    pair = swapped(pair)
    own = small(add_kernel, pltpu.VMEM(keep.shape, BF), keep, pair)
    pieces = own.reshape(size, own.shape[0] // size, own.shape[1])
    pieces = exchanged(pieces, GROUP)
    far, right = beside_in()
    own = repeated_sum(pieces, shares(FAR))
    pieces = exchanged(own, FAR)
    left = beside_far()
    own = repeated_sum(pieces, size)
    mine = exchanged(own, GROUP).reshape(keep.shape)
    _, bound, half = right.shape
    outs = [jax.ShapeDtypeStruct((4 * bound, half), BF)] * 4
    outs = small(join_kernel, outs, core, pair, far, right, left)
    mine, *outs = lax.optimization_barrier((mine, *outs))
    other = swapped(mine)
    return mine, other, [out[None, None] for out in outs]


def shifted(block, axis, step):
    size = lax.axis_size(axis)
    pairs = [(i, i + step) for i in range(size) if 0 <= i + step < size]
    return lax.ppermute(block, axis, pairs)


def across_chips(block):
    size = lax.axis_size(ROW)
    up = [(i, i + 1) for i in range(1, size - 1, 2)]
    return lax.ppermute(block, ROW, up + [(j, i) for i, j in up])


def per_device(
    features,
    local_mask,
    halo_mask,
    boundary_index,
    labels,
    halo_first,
    halo_second,
    halo_third,
    return_second,
    return_third,
    weight_first,
    weight_second,
    weight_third,
):
    core = lax.axis_index(PAIR).astype(jnp.int32).reshape(1)
    keep, pair, far, left, right = step(
        core,
        boundary_index[0],
        labels[0],
        features[0, 0].T,
        local_mask[0, 0],
        halo_mask[0, 0],
        halo_first[0, 0].T,
        halo_second[0, 0],
        halo_third[0, 0],
        return_second[0, 0],
        return_third[0, 0],
        weight_first,
        weight_second,
        weight_third.T,
    )

    def beside_in():
        return across_chips(far), shifted(right, COL, 1)

    def beside_far():
        return shifted(left, COL, -1)

    one, two, three = weight_first.shape[0], weight_second.shape[0], weight_third.shape[1]
    mine, other, outs = total_of(core, keep, pair, beside_in, beside_far)
    next_second, next_third, back_second, back_third = outs
    grad_one, grad_two, grad_three = unpack(core, mine, other, one, two, three)
    grad_three = grad_three.T
    return (grad_one, grad_two, grad_three, next_second, next_third, back_second, back_third)


def solution(mesh):
    torus = Mesh(mesh.devices.reshape(8, 2, 4, 4), ("row_0", "row_1", "col_0", "col_1"))
    in_specs = (
        P(ROW, COL, None, None),
        P(ROW, COL, None, None),
        P(ROW, COL, None, None),
        P(ROW, COL, None),
        P(ROW, COL, None),
        P(ROW, COL, None, None),
        P(ROW, COL, None, None),
        P(ROW, COL, None, None),
        P(ROW, COL, None, None),
        P(ROW, COL, None, None),
        P(),
        P(),
        P(),
    )
    out_specs = (
        P(),
        P(),
        P(),
        P(ROW, COL, None, None),
        P(ROW, COL, None, None),
        P(ROW, COL, None, None),
        P(ROW, COL, None, None),
    )
    return jax.shard_map(
        per_device, mesh=torus, in_specs=in_specs, out_specs=out_specs, check_vma=False
    )
```

```python
import jax
import jax.numpy as jnp
from jax import lax
from jax.experimental import pallas as pl
from jax.experimental.pallas import tpu as pltpu
from jax.sharding import Mesh
from jax.sharding import PartitionSpec as P


ROW = ("row_0", "row_1")
COL = ("col_0", "col_1")


def dot(a, b, contract=(1, 0)):
    dims = (((contract[0],), (contract[1],)), ((), ()))
    return lax.dot_general(a, b, dims, preferred_element_type=jnp.float32)


def silu_of(pre):
    return pre / (1.0 + jnp.exp(-pre))


def slope(pre):
    sigma = 1.0 / (1.0 + jnp.exp(-pre))
    return sigma * (1.0 + pre * (1.0 - sigma))


BF = jnp.bfloat16
F32 = jnp.float32
CHUNKS = 4
ROWS = 1024


def padded_up(size):
    return size + (-size) % 128


def step_kernel(
    core_ref, index_ref, label_ref, features, local_mask, halo_mask, halo_first, halo_second, halo_third,
    return_second, return_third, weight_first, weight_second, weight_third,
    keep_out, pair_out, far_out, left_out, right_out,
    feat_t, local_raw, halo_raw, first_t, second, third, ret_two, ret_three, w_one, w_two, w_three,
    local, halo, hits, inverse, mixed_one, mixed_two, mixed_three, pre_one, pre_two,
    hidden_one, hidden_two, scaled, packed, upright, sends, feat, first, in_sem, local_sem, halo_sem, out_sem,
):
    nodes, wide = feat.shape
    rows = nodes // CHUNKS
    bound = hits.shape[1] // 4

    def fetch(source, target, sem):
        copy = pltpu.make_async_copy(source, target, sem)
        copy.start()
        return copy

    def part(ref, c):
        return ref.at[pl.ds(c * rows, rows)]

    got_feat = fetch(features, feat_t, in_sem.at[0])
    got_first = fetch(halo_first, first_t, in_sem.at[1])
    got_local, got_halo = [], []
    for c in range(CHUNKS):
        got_local.append(fetch(part(local_mask, c), part(local_raw, c), local_sem.at[c]))
        got_halo.append(fetch(part(halo_mask, c), part(halo_raw, c), halo_sem.at[c]))
    rest = [
        fetch(source, target, in_sem.at[2 + n])
        for n, (source, target) in enumerate(
            (
                (weight_first, w_one), (weight_second, w_two), (halo_second, second),
                (weight_third, w_three), (halo_third, third),
                (return_third, ret_three), (return_second, ret_two),
            )
        )
    ]
    got_w_one, got_w_two, got_second, got_w_three, got_third, got_ret_three, got_ret_two = rest

    hits[...] = (
        lax.broadcasted_iota(jnp.int32, hits.shape, 0) == index_ref[...]
    ).astype(F32).astype(BF)

    got_feat.wait()
    feat[...] = jnp.transpose(feat_t[...])
    got_first.wait()
    first[...] = jnp.transpose(first_t[...])
    for c in range(CHUNKS):
        at = pl.ds(c * rows, rows)
        got_local[c].wait()
        got_halo[c].wait()
        raw_local = local_raw[at, :].astype(F32)
        raw_halo = halo_raw[at, :].astype(F32)
        local[at, :] = raw_local.astype(BF)
        halo[at, :] = raw_halo.astype(BF)
        degree = (
            1.0 + jnp.sum(raw_local, axis=1, keepdims=True) + jnp.sum(raw_halo, axis=1, keepdims=True)
        )
        inverse[at, :] = 1.0 / degree
        summed = dot(local[at, :], feat[...]) + feat[at, :].astype(F32) + dot(halo[at, :], first[...])
        mixed_one[at, :] = (summed * inverse[at, :]).astype(BF)
        if c == 0:
            got_w_one.wait()
        pre = dot(mixed_one[at, :], w_one[...])
        pre_one[at, :] = pre
        hidden_one[at, :] = silu_of(pre).astype(BF)

    half = packed.shape[2]
    core = core_ref[0]
    out = []

    def place(array, n):
        for k in range(2):
            for h in range(2):
                upright[k, pl.ds((2 * n + h) * bound, bound), :] = array[
                    k * bound : (k + 1) * bound, h * half : (h + 1) * half
                ].astype(BF)
            sends[k, n] = array[(2 + k) * bound : (3 + k) * bound].astype(BF)

    def spread(values, remote, mixed):
        for c in range(CHUNKS):
            at = pl.ds(c * rows, rows)
            summed = dot(local[at, :], values[...]) + values[at, :].astype(F32) + dot(halo[at, :], remote[...])
            mixed[at, :] = (summed * inverse[at, :]).astype(BF)

    got_w_two.wait()
    got_second.wait()
    spread(hidden_one, second, mixed_two)
    pre = dot(mixed_two[...], w_two[...])
    pre_two[...] = pre
    hidden_two[...] = silu_of(pre).astype(BF)

    got_w_three.wait()
    got_third.wait()
    spread(hidden_two, third, mixed_three)
    logits = dot(mixed_three[...], w_three[...], (1, 1))
    expo = jnp.exp(logits)
    probs = expo / jnp.sum(expo, axis=1, keepdims=True)
    target = jnp.transpose(
        (lax.broadcasted_iota(jnp.int32, (128, nodes), 0) == label_ref[...]).astype(F32)
    )[:, : logits.shape[1]]
    up_three = ((probs - target) / nodes).astype(BF)

    def retract(across, returned):
        scaled[...] = (across * inverse[...]).astype(BF)
        carried = dot(local[...], scaled[...], (0, 0)) + scaled[...].astype(F32)
        return carried + dot(hits[...], returned[...])

    got_ret_three.wait()
    got_ret_two.wait()
    two = w_two.shape[0]
    third_at = two + padded_up(wide)
    tail = two + wide // 16 * 16
    for h in range(2):
        packed[h, pl.ds(tail, ROWS - tail), :] = jnp.zeros((ROWS - tail, half), BF)

    def pack(row, grad):
        for h in range(2):
            packed[h, pl.ds(row, grad.shape[0]), :] = grad[:, h * half : (h + 1) * half].astype(BF)

    pack(third_at, dot(up_three, mixed_three[...], (0, 0)))
    carried = retract(dot(up_three, w_three[...]), ret_three)
    place(dot(halo[...], scaled[...], (0, 0)), 3)
    place(dot(hits[...], hidden_one[...], (0, 0)), 0)
    place(dot(hits[...], hidden_two[...], (0, 0)), 1)
    up_two = (carried * slope(pre_two[...])).astype(BF)
    pack(0, dot(mixed_two[...], up_two, (0, 0)))
    carried = retract(dot(up_two, w_two[...], (1, 1)), ret_two)
    up_one = (carried * slope(pre_one[...])).astype(BF)
    pack(two, dot(mixed_one[...], up_one, (0, 0)))
    place(dot(halo[...], scaled[...], (0, 0)), 2)
    out.append(fetch(packed.at[1 - core], pair_out.at[0], out_sem.at[4]))
    out.append(fetch(packed.at[core], keep_out, out_sem.at[5]))
    out += [
        fetch(upright.at[1 - core], pair_out.at[1], out_sem.at[0]),
        fetch(upright.at[core], far_out, out_sem.at[1]),
        fetch(sends.at[0], left_out, out_sem.at[2]),
        fetch(sends.at[1], right_out, out_sem.at[3]),
    ]
    for copy in out:
        copy.wait()


def step(core, index, labels, *arrays):
    (features, _, _, _, halo_second, _,
     _, _, _, _, _) = arrays
    depth, nodes = features.shape
    wide = depth
    slots, hidden = halo_second.shape
    v = pltpu.VMEM
    scratch = [v(a.shape, a.dtype) for a in arrays]
    scratch += [
        v((nodes, nodes), BF), v((nodes, slots), BF), v((nodes, slots), BF), v((nodes, 1), F32),
        v((nodes, wide), BF), v((nodes, hidden), BF), v((nodes, hidden), BF),
        v((nodes, hidden), F32), v((nodes, hidden), F32),
        v((nodes, hidden), BF), v((nodes, hidden), BF), v((nodes, hidden), BF),
        v((2, ROWS, hidden // 2), BF), v((2, 2 * slots, hidden // 2), BF),
        v((2, 4, slots // 4, hidden), BF),
        v((nodes, wide), BF), v((slots, wide), BF),
        pltpu.SemaphoreType.DMA((9,)), pltpu.SemaphoreType.DMA((CHUNKS,)),
        pltpu.SemaphoreType.DMA((CHUNKS,)), pltpu.SemaphoreType.DMA((6,)),
    ]
    half = v((ROWS, hidden // 2), BF)
    block = v((4, slots // 4, hidden), BF)
    return pl.pallas_call(
        step_kernel,
        out_shape=[half, v((2, ROWS, hidden // 2), BF), half, block, block],
        in_specs=[pl.BlockSpec(memory_space=pltpu.SMEM)]
        + [pl.BlockSpec(memory_space=pltpu.VMEM)] * 2
        + [pl.BlockSpec(memory_space=pltpu.HBM)] * len(arrays),
        out_specs=[pl.BlockSpec(memory_space=pl.ANY)] * 5,
        scratch_shapes=scratch,
        compiler_params=pltpu.CompilerParams(vmem_limit_bytes=62_000_000),
        cost_estimate=pl.CostEstimate(flops=8_000_000_000, bytes_accessed=12_000_000, transcendentals=1_000_000),
        name="step",
    )(core, index, labels, *arrays)


def small(kernel, out_shape, *arrays):
    scalars = sum(a.ndim == 1 for a in arrays)
    return pl.pallas_call(
        kernel,
        out_shape=out_shape,
        in_specs=[pl.BlockSpec(memory_space=pltpu.SMEM)] * scalars
        + [pl.BlockSpec(memory_space=pltpu.VMEM)] * (len(arrays) - scalars),
        out_specs=jax.tree.map(lambda _: pl.BlockSpec(memory_space=pltpu.VMEM), out_shape),
        compiler_params=pltpu.CompilerParams(vmem_limit_bytes=8 * 2**20),
        cost_estimate=pl.CostEstimate(flops=500_000, bytes_accessed=1_000_000, transcendentals=0),
    )(*arrays)


def add_kernel(keep, pair, out):
    out[...] = (keep[...].astype(F32) + pair[0].astype(F32)).astype(BF)


def sum_kernel(pieces, out):
    total = pieces[0].astype(F32)
    for n in range(1, pieces.shape[0]):
        total = total + pieces[n].astype(F32)
    total = total.astype(BF)
    for n in range(out.shape[0]):
        out[n] = total


def repeated_sum(pieces, count):
    return small(sum_kernel, pltpu.VMEM((count, *pieces.shape[1:]), BF), pieces)


def join_kernel(core_ref, pair, far, right, left, *outs):
    upper = core_ref[0] == 0
    bound, half = right.shape[1], pair.shape[2]
    for n, out in enumerate(outs):
        for h in range(2):
            at = pl.ds((2 * n + h) * bound, bound)
            cols = slice(h * half, (h + 1) * half)
            near, away = pair[1, at, :], far[at, :]
            out[0:bound, cols] = jnp.where(upper, away, near)
            out[bound : 2 * bound, cols] = jnp.where(upper, near, away)
        out[2 * bound : 3 * bound, :] = right[n]
        out[3 * bound : 4 * bound, :] = left[n]


def unpack_kernel(core_ref, mine, other, one_out, two_out, three_out):
    own_left = core_ref[0] == 0
    half = mine.shape[1]

    def rows_of(row, count):
        a, b = mine[pl.ds(row, count), :].astype(F32), other[pl.ds(row, count), :].astype(F32)
        return jnp.where(own_left, a, b), jnp.where(own_left, b, a)

    row = 0
    for out in (two_out, one_out, three_out):
        for h, part in enumerate(rows_of(row, out.shape[0])):
            out[:, h * half : (h + 1) * half] = part
        row += out.shape[0] if out is two_out else padded_up(out.shape[0])


def unpack(core, mine, other, one, two, three):
    wide = mine.shape[1] * 2
    shapes = [jax.ShapeDtypeStruct((n, wide), F32) for n in (one, two, three)]
    return small(unpack_kernel, shapes, core, mine, other)


PAIR = "row_1"
GROUP = COL
FAR = ("row_0",)


def shares(axes):
    size = 1
    for axis in axes:
        size *= lax.axis_size(axis)
    return size


def exchanged(pieces, axes):
    return lax.all_to_all(pieces, axes, 0, 0, tiled=True)


def swapped(half):
    return lax.ppermute(half, PAIR, [(0, 1), (1, 0)])


def total_of(core, keep, pair, beside_in, beside_far):
    size = shares(GROUP)
    pair = swapped(pair)
    own = small(add_kernel, pltpu.VMEM(keep.shape, BF), keep, pair)
    pieces = own.reshape(size, own.shape[0] // size, own.shape[1])
    pieces = exchanged(pieces, GROUP)
    far = beside_in()
    own = repeated_sum(pieces, shares(FAR))
    pieces = exchanged(own, FAR)
    right, left = beside_far()
    own = repeated_sum(pieces, size)
    mine = exchanged(own, GROUP).reshape(keep.shape)
    other = swapped(mine)
    _, bound, half = right.shape
    outs = [jax.ShapeDtypeStruct((4 * bound, half), BF)] * 4
    outs = small(join_kernel, outs, core, pair, far, right, left)
    return mine, other, [out[None, None] for out in outs]


def shifted(block, axis, step):
    size = lax.axis_size(axis)
    pairs = [(i, i + step) for i in range(size) if 0 <= i + step < size]
    return lax.ppermute(block, axis, pairs)


def across_chips(block):
    size = lax.axis_size(ROW)
    up = [(i, i + 1) for i in range(1, size - 1, 2)]
    return lax.ppermute(block, ROW, up + [(j, i) for i, j in up])


def per_device(
    features,
    local_mask,
    halo_mask,
    boundary_index,
    labels,
    halo_first,
    halo_second,
    halo_third,
    return_second,
    return_third,
    weight_first,
    weight_second,
    weight_third,
):
    core = lax.axis_index(PAIR).astype(jnp.int32).reshape(1)
    keep, pair, far, left, right = step(
        core,
        boundary_index[0],
        labels[0],
        features[0, 0].T,
        local_mask[0, 0],
        halo_mask[0, 0],
        halo_first[0, 0].T,
        halo_second[0, 0],
        halo_third[0, 0],
        return_second[0, 0],
        return_third[0, 0],
        weight_first,
        weight_second,
        weight_third.T,
    )

    def beside_in():
        return across_chips(far)

    def beside_far():
        return shifted(right, COL, 1), shifted(left, COL, -1)

    one, two, three = weight_first.shape[0], weight_second.shape[0], weight_third.shape[1]
    mine, other, outs = total_of(core, keep, pair, beside_in, beside_far)
    next_second, next_third, back_second, back_third = outs
    grad_one, grad_two, grad_three = unpack(core, mine, other, one, two, three)
    grad_three = grad_three.T
    return (grad_one, grad_two, grad_three, next_second, next_third, back_second, back_third)


def solution(mesh):
    torus = Mesh(mesh.devices.reshape(8, 2, 4, 4), ("row_0", "row_1", "col_0", "col_1"))
    in_specs = (
        P(ROW, COL, None, None),
        P(ROW, COL, None, None),
        P(ROW, COL, None, None),
        P(ROW, COL, None),
        P(ROW, COL, None),
        P(ROW, COL, None, None),
        P(ROW, COL, None, None),
        P(ROW, COL, None, None),
        P(ROW, COL, None, None),
        P(ROW, COL, None, None),
        P(),
        P(),
        P(),
    )
    out_specs = (
        P(),
        P(),
        P(),
        P(ROW, COL, None, None),
        P(ROW, COL, None, None),
        P(ROW, COL, None, None),
        P(ROW, COL, None, None),
    )
    return jax.shard_map(
        per_device, mesh=torus, in_specs=in_specs, out_specs=out_specs, check_vma=False
    )
```
